256 devices in a mesh: param: 32 (over z, x), task: 8 (over y, core).
Axes of the slice: x: 4, y: 4, z: 8, core: 2. Of those that a mesh axis runs over, the one named last changes fastest.
Arguments:
- task_ids: int32 [1024], P('task'), may hold values from 0 to 2047
- task_table: bfloat16 [2048, 256], P('param'), may hold values from -12 to 12
- enc_in: bfloat16 [256, 512], replicated, may hold values from -0.375 to 0.375
- enc_out: bfloat16 [512, 256], replicated, may hold values from -0.25 to 0.25
- generator: bfloat16 [256, 8, 114688], P(None, None, ('param', 'task')), may hold values from -6 to 6
- gain: bfloat16 [8, 114688], P(None, ('param', 'task')), may hold values from 0.099609375 to 1.8984375
Outputs:
- adapters: bfloat16 [1024, 8, 114688], P(None, None, ('param', 'task'))
The draws below stay inside these ranges and needn't reach their ends.
Inputs may be any that keep to these rules, and one draw needn't show every extreme that they name: `task_ids`: each id names a row of task_table.
All inputs are finite; a program needn't handle non-finite values.
Results may differ from the reference program's by a relative error of at most 0.00055.
The reference program's roundings to bfloat16 on the way count: a program that leaves them out, or rounds other values in their place, can miss the bound.
Values may be sent and summed in bfloat16 or wider, within the bound.
No kernel may reach another device: no remote copies, remote signals or barrier semaphores. Data moves between devices by JAX's collectives and lax.ppermute only.
A program may use at most 64 MiB of HBM per device.

```python
import math
import jax
import jax.numpy as jnp
from jax import lax

EMB = 256
ENC = 512
LAYERS = 4
TASKS = 1024
TABLE = 2048
BLOCK = 114688


def draw_task_table(key, part):
    row_key, value_key = jax.random.split(jax.random.fold_in(key, 11), 2)
    scales = jnp.exp(jax.random.uniform(row_key, (TABLE, 1), jnp.float32, math.log(0.3), math.log(3.0)))
    values = jnp.clip(jax.random.normal(value_key, (TABLE, EMB), jnp.float32), -4.0, 4.0)
    return (scales * values).astype(jnp.bfloat16)


def draw_generator(key, part):
    column_key, value_key = jax.random.split(jax.random.fold_in(key, 23), 2)
    groups = 2 * LAYERS
    position = jnp.arange(BLOCK, dtype=jnp.int32).astype(jnp.float32)
    rising = jnp.exp(math.log(3.0) * position / BLOCK)
    spread = jnp.exp(jax.random.uniform(column_key, (groups, BLOCK), jnp.float32, 0.0, math.log(10.0)))
    scales = (0.05 * rising[None, :] * spread)[None, :, :]
    values = jnp.clip(jax.random.normal(value_key, (EMB, groups, BLOCK), jnp.float32), -4.0, 4.0)
    return (scales * values).astype(jnp.bfloat16)


def plant(result, own_key, low, high):
    spot = [jax.random.randint(jax.random.fold_in(own_key, axis), (), 0, length) for axis, length in enumerate(result.shape)]
    widest = result.shape.index(max(result.shape))
    neighbour = spot[:widest] + [(spot[widest] + 1) % result.shape[widest]] + spot[widest + 1:]
    return result.at[tuple(spot)].set(low).at[tuple(neighbour)].set(high)


def noise(own_key, dims, deviation, most, kind=jnp.bfloat16):
    return jnp.clip(deviation * jax.random.normal(own_key, dims, jnp.float32), -most, most).astype(kind)


def setup_inputs(seed: int = 0) -> dict:
    key_list = jax.random.split(jax.random.key(seed), 7)
    return {
        "task_ids": plant(jax.random.randint(key_list[0], (TASKS,), 0, TABLE), jax.random.fold_in(key_list[0], 1), 0, TABLE - 1).astype(jnp.int32),
        "task_table": draw_task_table(jax.random.fold_in(key_list[6], 71), 0),
        "enc_in": noise(key_list[2], (EMB, ENC), EMB ** -0.5, 0.375),
        "enc_out": noise(key_list[3], (ENC, EMB), ENC ** -0.5, 0.25),
        "generator": draw_generator(jax.random.fold_in(key_list[6], 71), 0),
        "gain": jnp.clip(1.0 + 0.18 * jax.random.normal(key_list[5], (2 * LAYERS, BLOCK), jnp.float32), 0.099609375, 1.8984375).astype(jnp.bfloat16),
    }


EPSILON = 1e-06

def encode(raw_rows, enc_in, enc_out):
    inner_act = jax.nn.gelu(jnp.dot(raw_rows, enc_in, preferred_element_type=jnp.float32)).astype(jnp.bfloat16)
    mixed_sum = raw_rows.astype(jnp.float32) + jnp.dot(inner_act, enc_out, preferred_element_type=jnp.float32)
    return mixed_sum.astype(jnp.bfloat16)

def reference(task_ids, task_table, enc_in, enc_out, generator, gain):
    raw_rows = jnp.take(task_table, task_ids.astype(jnp.int32), axis=0)
    embedded = encode(raw_rows, enc_in, enc_out)
    weight_blocks = generator.transpose(1, 0, 2)

    def normalize(operands):
        weights, gain_part = operands
        generated = jnp.dot(embedded, weights, preferred_element_type=jnp.float32)
        mean_power = lax.optimization_barrier(jnp.mean(generated * generated, axis=1, keepdims=True))
        scaled = generated * lax.rsqrt(mean_power + EPSILON) * gain_part.astype(jnp.float32)[None, :]
        return scaled.astype(jnp.bfloat16)
    stacked = lax.map(normalize, (weight_blocks, gain))
    return stacked.transpose(1, 0, 2)
```

```python
import jax
import jax.numpy as jnp
from jax import lax
from jax.experimental import pallas as pl
from jax.experimental.pallas import tpu as pltpu
from jax.sharding import Mesh
from jax.sharding import PartitionSpec as P

BLOCK = 114688
PARAM = ("z", "x")
TASK = ("y", "core")
PARAM_TASK = ("z", "x", "y", "core")
LANES = 128
EPSILON = 1e-06

VMEM = pl.BlockSpec(memory_space=pltpu.VMEM)
HBM = pl.BlockSpec(memory_space=pltpu.HBM)
SMEM = pl.BlockSpec(memory_space=pltpu.SMEM)


def copy_for_each(x, axis):
    copies = jnp.broadcast_to(x, (lax.axis_size(axis), *x.shape))
    return lax.all_to_all(copies, axis, split_axis=0, concat_axis=0, tiled=True)


def encode_kernel(core_ref, table_hbm, enc_in_hbm, enc_out_hbm, out_ref, table_ref, enc_in_ref, enc_out_ref, sems):
    copies, rows, _ = out_ref.shape
    start = pl.multiple_of(core_ref[0] * rows, rows)
    loads = [
        pltpu.make_async_copy(table_hbm.at[pl.ds(start, rows), :], table_ref, sems.at[0]),
        pltpu.make_async_copy(enc_in_hbm, enc_in_ref, sems.at[1]),
        pltpu.make_async_copy(enc_out_hbm, enc_out_ref, sems.at[2]),
    ]
    for load in loads:
        load.start()
    loads[0].wait()
    loads[1].wait()
    raw = table_ref[...]
    inner = jax.nn.gelu(jnp.dot(raw, enc_in_ref[...], preferred_element_type=jnp.float32)).astype(jnp.bfloat16)
    loads[2].wait()
    mixed = raw.astype(jnp.float32) + jnp.dot(inner, enc_out_ref[...], preferred_element_type=jnp.float32)
    encoded = mixed.astype(jnp.bfloat16)
    for copy in range(copies):
        out_ref[copy] = encoded


def encode_half(core, task_table, enc_in, enc_out, copies):
    rows, width = task_table.shape[0] // 2, task_table.shape[1]
    return pl.pallas_call(
        encode_kernel,
        out_shape=jax.ShapeDtypeStruct((copies, rows, width), jnp.bfloat16),
        in_specs=[SMEM, HBM, HBM, HBM],
        out_specs=VMEM,
        scratch_shapes=[
            pltpu.VMEM((rows, width), jnp.bfloat16),
            pltpu.VMEM(enc_in.shape, jnp.bfloat16),
            pltpu.VMEM(enc_out.shape, jnp.bfloat16),
            pltpu.SemaphoreType.DMA((3,)),
        ],
        compiler_params=pltpu.CompilerParams(vmem_limit_bytes=8 << 20),
        name="encode_half",
    )(core, task_table, enc_in, enc_out)


def squares_kernel(
    core_ref, ids_ref, mine_ref, other_ref, weights_hbm, embedded_ref, squares_ref, weights_ref, sem, *, shard
):
    load = pltpu.make_async_copy(weights_hbm, weights_ref, sem)
    load.start()
    chunks, groups, lanes = squares_ref.shape
    rows = mine_ref.shape[0]
    half = shard // 2
    columns = weights_ref.shape[0] // groups
    core = core_ref[0]
    ids = jnp.transpose(ids_ref[...])
    place = lax.broadcasted_iota(jnp.int32, (1, rows), 1)
    base = (place // half) * shard + place % half

    def picked(part_ref, which):
        labels = base + which * half
        hot = [(ids[:, k : k + 1] == labels).astype(jnp.bfloat16) for k in range(chunks)]
        return jnp.dot(jnp.concatenate(hot, axis=0), part_ref[...], preferred_element_type=jnp.float32)

    embedded = (picked(mine_ref, core) + picked(other_ref, 1 - core)).astype(jnp.bfloat16)
    embedded_ref[...] = embedded
    load.wait()
    for g in range(groups):
        made = lax.dot_general(
            weights_ref[g * columns : (g + 1) * columns, :],
            embedded,
            (((1,), (1,)), ((), ())),
            preferred_element_type=jnp.float32,
        )
        total = jnp.sum(made * made, axis=0, keepdims=True)
        for k in range(chunks):
            squares_ref[k, g : g + 1, :] = total[:, k * lanes : (k + 1) * lanes]


def squares_of(core, ids, mine, other, weights, groups, shard):
    chunks, lanes = ids.shape
    return pl.pallas_call(
        lambda *refs: squares_kernel(*refs, shard=shard),
        out_shape=(
            jax.ShapeDtypeStruct((chunks * lanes, mine.shape[1]), jnp.bfloat16),
            jax.ShapeDtypeStruct((chunks, groups, lanes), jnp.float32),
        ),
        in_specs=[SMEM, VMEM, VMEM, VMEM, HBM],
        out_specs=(VMEM, VMEM),
        scratch_shapes=[pltpu.VMEM(weights.shape, weights.dtype), pltpu.SemaphoreType.DMA],
        compiler_params=pltpu.CompilerParams(vmem_limit_bytes=24 << 20),
        name="squares",
    )(core, ids, mine, other, weights)


def scale_kernel(weights_ref, embedded_ref, totals_ref, gain_ref, out_ref):
    g = pl.program_id(0)
    chunks = totals_ref.shape[0]
    power = jnp.concatenate([totals_ref[k, pl.ds(g, 1), :] for k in range(chunks)], axis=1)
    inverse = lax.rsqrt(power / BLOCK + EPSILON)
    made = lax.dot_general(
        weights_ref[...], embedded_ref[...], (((1,), (1,)), ((), ())), preferred_element_type=jnp.float32
    )
    out_ref[...] = (made * inverse * gain_ref[...].astype(jnp.float32)).astype(jnp.bfloat16)


def scaled_adapters(weights, embedded, totals, gain):
    chunks, groups, lanes = totals.shape
    columns = weights.shape[0] // groups
    tasks, width = embedded.shape
    return pl.pallas_call(
        scale_kernel,
        grid=(groups,),
        out_shape=jax.ShapeDtypeStruct((groups * columns, tasks), jnp.bfloat16),
        in_specs=[
            pl.BlockSpec((columns, width), lambda g: (g, 0)),
            pl.BlockSpec((tasks, width), lambda g: (0, 0)),
            pl.BlockSpec((chunks, groups, lanes), lambda g: (0, 0, 0)),
            pl.BlockSpec((columns, 1), lambda g: (g, 0)),
        ],
        out_specs=pl.BlockSpec((columns, tasks), lambda g: (g, 0)),
        compiler_params=pltpu.CompilerParams(vmem_limit_bytes=24 << 20),
        name="scale",
    )(weights, embedded, totals, gain)


def on_device(task_ids, task_table, enc_in, enc_out, generator, gain):
    width, groups, columns = generator.shape
    shard = task_table.shape[0]
    core = lax.axis_index("core").reshape(1).astype(jnp.int32)
    weights = generator.transpose(1, 2, 0).reshape(groups * columns, width)
    copies = encode_half(core, task_table, enc_in, enc_out, lax.axis_size(PARAM))
    mine = lax.all_to_all(copies, PARAM, split_axis=0, concat_axis=0, tiled=True).reshape(-1, width)
    ids = copy_for_each(task_ids, TASK)
    mine, ids = lax.optimization_barrier((mine, ids))
    other = lax.ppermute(mine, "core", [(0, 1), (1, 0)])
    embedded, squares = squares_of(core, ids, mine, other, weights, groups, shard)
    spread = lax.all_to_all(squares, TASK, split_axis=0, concat_axis=0, tiled=True)
    totals = copy_for_each(spread.sum(axis=0), PARAM).sum(axis=0)
    totals = copy_for_each(totals, TASK)
    gain_column = gain.reshape(groups * columns, 1)
    made = scaled_adapters(weights, embedded, totals, gain_column)
    return made.reshape(groups, columns, -1).transpose(2, 0, 1)


def solution(mesh):
    torus = Mesh(mesh.devices.reshape(8, 4, 4, 2), PARAM_TASK)
    return jax.shard_map(
        on_device,
        mesh=torus,
        in_specs=(
            P(TASK),
            P(PARAM, None),
            P(),
            P(),
            P(None, None, PARAM_TASK),
            P(None, PARAM_TASK),
        ),
        out_specs=P(None, None, PARAM_TASK),
        check_vma=False,
    )
```

```python
import jax
import jax.numpy as jnp
from jax import lax
from jax.experimental import pallas as pl
from jax.experimental.pallas import tpu as pltpu
from jax.sharding import Mesh
from jax.sharding import PartitionSpec as P

BLOCK = 114688
PARAM = ("z", "x")
TASK = ("y", "core")
PARAM_TASK = ("z", "x", "y", "core")
LANES = 128
EPSILON = 1e-06

VMEM = pl.BlockSpec(memory_space=pltpu.VMEM)
HBM = pl.BlockSpec(memory_space=pltpu.HBM)
SMEM = pl.BlockSpec(memory_space=pltpu.SMEM)
ROWS_BY_ROWS = (((1,), (1,)), ((), ()))


def in_hbm(x):
    return pltpu.with_memory_space_constraint(x, pltpu.HBM)


def limit(mebibytes):
    return pltpu.CompilerParams(vmem_limit_bytes=mebibytes << 20)


def exchange(x, axis):
    return lax.all_to_all(x, axis, split_axis=0, concat_axis=0, tiled=True)


def copy_for_each(x, axis):
    return exchange(jnp.broadcast_to(x, (lax.axis_size(axis), *x.shape)), axis)


def encode_kernel(core_ref, table_hbm, enc_in_hbm, enc_out_hbm, out_ref, table_ref, enc_in_ref, enc_out_ref, sems):
    copies, rows, _ = out_ref.shape
    start = pl.multiple_of(core_ref[0] * rows, rows)
    loads = [
        pltpu.make_async_copy(table_hbm.at[pl.ds(start, rows), :], table_ref, sems.at[0]),
        pltpu.make_async_copy(enc_in_hbm, enc_in_ref, sems.at[1]),
        pltpu.make_async_copy(enc_out_hbm, enc_out_ref, sems.at[2]),
    ]
    for load in loads:
        load.start()
    loads[0].wait()
    loads[1].wait()
    raw = table_ref[...]
    inner = jax.nn.gelu(jnp.dot(raw, enc_in_ref[...], preferred_element_type=jnp.float32)).astype(jnp.bfloat16)
    loads[2].wait()
    mixed = raw.astype(jnp.float32) + jnp.dot(inner, enc_out_ref[...], preferred_element_type=jnp.float32)
    encoded = mixed.astype(jnp.bfloat16)
    for copy in range(copies):
        out_ref[copy] = encoded


def encode_half(core, task_table, enc_in, enc_out, copies):
    rows, width = task_table.shape[0] // 2, task_table.shape[1]
    return pl.pallas_call(
        encode_kernel,
        out_shape=jax.ShapeDtypeStruct((copies, rows, width), jnp.bfloat16),
        in_specs=[SMEM, HBM, HBM, HBM],
        out_specs=VMEM,
        scratch_shapes=[
            pltpu.VMEM((rows, width), jnp.bfloat16),
            pltpu.VMEM(enc_in.shape, jnp.bfloat16),
            pltpu.VMEM(enc_out.shape, jnp.bfloat16),
            pltpu.SemaphoreType.DMA((3,)),
        ],
        compiler_params=limit(8),
        name="encode_half",
    )(core, in_hbm(task_table), in_hbm(enc_in), in_hbm(enc_out))


def picked_rows(ids_ref, part_ref, which, half):
    chunks = ids_ref.shape[0]
    ids = jnp.transpose(ids_ref[...])
    place = lax.broadcasted_iota(jnp.int32, (1, part_ref.shape[0]), 1)
    labels = (place // half) * (2 * half) + place % half + which * half
    hot = [(ids[:, k : k + 1] == labels).astype(jnp.bfloat16) for k in range(chunks)]
    return jnp.dot(jnp.concatenate(hot, axis=0), part_ref[...], preferred_element_type=jnp.float32)


def first_half(core, ids, mine, weights, half):
    def kernel(core_ref, ids_ref, mine_ref, weights_hbm, part_ref, weights_ref, sem):
        load = pltpu.make_async_copy(weights_hbm, weights_ref, sem)
        load.start()
        part_ref[...] = picked_rows(ids_ref, mine_ref, core_ref[0], half).astype(jnp.bfloat16)
        load.wait()

    return pl.pallas_call(
        kernel,
        out_shape=(
            jax.ShapeDtypeStruct((ids.size, mine.shape[1]), jnp.bfloat16),
            jax.ShapeDtypeStruct(weights.shape, weights.dtype),
        ),
        in_specs=[SMEM, VMEM, VMEM, HBM],
        out_specs=(VMEM, VMEM),
        scratch_shapes=[pltpu.SemaphoreType.DMA],
        compiler_params=limit(16),
        name="first_half",
    )(core, ids, mine, in_hbm(weights))


def squares_of(core, ids, part, other, weights, groups, half):
    chunks, lanes = ids.shape
    columns = weights.shape[0] // groups

    def kernel(core_ref, ids_ref, part_ref, other_ref, weights_ref, embedded_ref, squares_ref):
        rest = picked_rows(ids_ref, other_ref, 1 - core_ref[0], half)
        embedded = (part_ref[...].astype(jnp.float32) + rest).astype(jnp.bfloat16)
        embedded_ref[...] = embedded
        for g in range(groups):
            made = lax.dot_general(
                weights_ref[g * columns : (g + 1) * columns, :],
                embedded,
                ROWS_BY_ROWS,
                preferred_element_type=jnp.float32,
            )
            total = jnp.sum(made * made, axis=0, keepdims=True)
            for k in range(chunks):
                squares_ref[k, g : g + 1, :] = total[:, k * lanes : (k + 1) * lanes]

    return pl.pallas_call(
        kernel,
        out_shape=(
            jax.ShapeDtypeStruct(part.shape, jnp.bfloat16),
            jax.ShapeDtypeStruct((chunks, groups, lanes), jnp.float32),
        ),
        in_specs=[SMEM, VMEM, VMEM, VMEM, VMEM],
        out_specs=(VMEM, VMEM),
        compiler_params=limit(24),
        name="squares",
    )(core, ids, part, other, weights)


def scaled_adapters(weights, embedded, totals, gain):
    chunks, groups, lanes = totals.shape
    columns = weights.shape[0] // groups
    tasks, width = embedded.shape
    padding = -columns % LANES

    def kernel(weights_ref, embedded_ref, totals_ref, gain_ref, out_hbm, out_ref, sems):
        gains = gain_ref[...].astype(jnp.float32)
        gains = jnp.transpose(jnp.concatenate([gains, jnp.zeros((groups, padding), jnp.float32)], axis=1))
        stores = []
        for g in range(groups):
            rows = pl.ds(g * columns, columns)
            power = jnp.concatenate([totals_ref[k, g : g + 1, :] for k in range(chunks)], axis=1)
            inverse = lax.rsqrt(power / BLOCK + EPSILON)
            made = lax.dot_general(
                weights_ref[g * columns : (g + 1) * columns, :],
                embedded_ref[...],
                ROWS_BY_ROWS,
                preferred_element_type=jnp.float32,
            )
            out_ref[g] = (made * inverse * gains[:columns, g : g + 1]).astype(jnp.bfloat16)
            store = pltpu.make_async_copy(out_ref.at[g], out_hbm.at[rows, :], sems.at[g])
            store.start()
            stores.append(store)
        for store in stores:
            store.wait()

    return pl.pallas_call(
        kernel,
        out_shape=jax.ShapeDtypeStruct((groups * columns, tasks), jnp.bfloat16),
        in_specs=[VMEM, VMEM, VMEM, VMEM],
        out_specs=HBM,
        scratch_shapes=[pltpu.VMEM((groups, columns, tasks), jnp.bfloat16), pltpu.SemaphoreType.DMA((groups,))],
        compiler_params=limit(24),
        name="scale",
    )(weights, embedded, totals, gain)


def on_device(task_ids, task_table, enc_in, enc_out, generator, gain):
    width, groups, columns = generator.shape
    half = task_table.shape[0] // 2
    core = lax.axis_index("core").reshape(1).astype(jnp.int32)
    weights = generator.transpose(1, 2, 0).reshape(groups * columns, width)
    copies = encode_half(core, task_table, enc_in, enc_out, lax.axis_size(PARAM))
    task_ids, copies = lax.optimization_barrier((task_ids, copies))
    mine = exchange(copies, PARAM).reshape(-1, width)
    ids = lax.all_gather(task_ids.reshape(1, -1), TASK, axis=0, tiled=True)
    mine, ids = lax.optimization_barrier((mine, ids))
    other = lax.ppermute(mine, "core", [(0, 1), (1, 0)])
    part, weights = first_half(core, ids, mine, weights, half)
    embedded, squares = squares_of(core, ids, part, other, weights, groups, half)
    totals = copy_for_each(exchange(squares, TASK).sum(axis=0), PARAM).sum(axis=0)
    totals = copy_for_each(totals, TASK)
    made = scaled_adapters(weights, embedded, totals, gain)
    return made.reshape(groups, columns, -1).transpose(2, 0, 1)


def solution(mesh):
    torus = Mesh(mesh.devices.reshape(8, 4, 4, 2), PARAM_TASK)
    return jax.shard_map(
        on_device,
        mesh=torus,
        in_specs=(
            P(TASK),
            P(PARAM, None),
            P(),
            P(),
            P(None, None, PARAM_TASK),
            P(None, PARAM_TASK),
        ),
        out_specs=P(None, None, PARAM_TASK),
        check_vma=False,
    )
```

```python
import jax
import jax.numpy as jnp
from jax import lax
from jax.experimental import pallas as pl
from jax.experimental.pallas import tpu as pltpu
from jax.sharding import Mesh
from jax.sharding import PartitionSpec as P

BLOCK = 114688
PARAM = ("z", "x")
TASK = ("y", "core")
PARAM_TASK = ("z", "x", "y", "core")
LANES = 128
EPSILON = 1e-06

VMEM = pl.BlockSpec(memory_space=pltpu.VMEM)
HBM = pl.BlockSpec(memory_space=pltpu.HBM)
SMEM = pl.BlockSpec(memory_space=pltpu.SMEM)
ROWS_BY_ROWS = (((1,), (1,)), ((), ()))


def in_hbm(x):
    return pltpu.with_memory_space_constraint(x, pltpu.HBM)


def limit(mebibytes):
    return pltpu.CompilerParams(vmem_limit_bytes=mebibytes << 20)


def exchange(x, axis):
    return lax.all_to_all(x, axis, split_axis=0, concat_axis=0, tiled=True)


def copy_for_each(x, axis):
    return exchange(jnp.broadcast_to(x, (lax.axis_size(axis), *x.shape)), axis)


def encode_kernel(core_ref, table_hbm, enc_in_hbm, enc_out_hbm, out_ref, table_ref, enc_in_ref, enc_out_ref, sems):
    copies, rows, _ = out_ref.shape
    start = pl.multiple_of(core_ref[0] * rows, rows)
    loads = [
        pltpu.make_async_copy(table_hbm.at[pl.ds(start, rows), :], table_ref, sems.at[0]),
        pltpu.make_async_copy(enc_in_hbm, enc_in_ref, sems.at[1]),
        pltpu.make_async_copy(enc_out_hbm, enc_out_ref, sems.at[2]),
    ]
    for load in loads:
        load.start()
    loads[0].wait()
    loads[1].wait()
    raw = table_ref[...]
    inner = jax.nn.gelu(jnp.dot(raw, enc_in_ref[...], preferred_element_type=jnp.float32)).astype(jnp.bfloat16)
    loads[2].wait()
    mixed = raw.astype(jnp.float32) + jnp.dot(inner, enc_out_ref[...], preferred_element_type=jnp.float32)
    encoded = mixed.astype(jnp.bfloat16)
    for copy in range(copies):
        out_ref[copy] = encoded


def encode_half(core, task_table, enc_in, enc_out, copies):
    rows, width = task_table.shape[0] // 2, task_table.shape[1]
    return pl.pallas_call(
        encode_kernel,
        out_shape=jax.ShapeDtypeStruct((copies, rows, width), jnp.bfloat16),
        in_specs=[SMEM, HBM, HBM, HBM],
        out_specs=VMEM,
        scratch_shapes=[
            pltpu.VMEM((rows, width), jnp.bfloat16),
            pltpu.VMEM(enc_in.shape, jnp.bfloat16),
            pltpu.VMEM(enc_out.shape, jnp.bfloat16),
            pltpu.SemaphoreType.DMA((3,)),
        ],
        compiler_params=limit(8),
        name="encode_half",
    )(core, in_hbm(task_table), in_hbm(enc_in), in_hbm(enc_out))


def picked_rows(ids_ref, part_ref, which, half):
    chunks = ids_ref.shape[0]
    ids = jnp.transpose(ids_ref[...])
    place = lax.broadcasted_iota(jnp.int32, (1, part_ref.shape[0]), 1)
    labels = (place // half) * (2 * half) + place % half + which * half
    hot = [(ids[:, k : k + 1] == labels).astype(jnp.bfloat16) for k in range(chunks)]
    return jnp.dot(jnp.concatenate(hot, axis=0), part_ref[...], preferred_element_type=jnp.float32)


def first_half(core, ids, mine, weights, half):
    def kernel(core_ref, ids_ref, mine_ref, weights_hbm, part_ref, weights_ref, sem):
        load = pltpu.make_async_copy(weights_hbm, weights_ref, sem)
        load.start()
        part_ref[...] = picked_rows(ids_ref, mine_ref, core_ref[0], half).astype(jnp.bfloat16)
        load.wait()

    return pl.pallas_call(
        kernel,
        out_shape=(
            jax.ShapeDtypeStruct((ids.size, mine.shape[1]), jnp.bfloat16),
            jax.ShapeDtypeStruct(weights.shape, weights.dtype),
        ),
        in_specs=[SMEM, VMEM, VMEM, HBM],
        out_specs=(VMEM, VMEM),
        scratch_shapes=[pltpu.SemaphoreType.DMA],
        compiler_params=limit(16),
        name="first_half",
    )(core, ids, mine, in_hbm(weights))


def embed(core, ids, part, other, half):
    def kernel(core_ref, ids_ref, part_ref, other_ref, embedded_ref):
        rest = picked_rows(ids_ref, other_ref, 1 - core_ref[0], half)
        embedded_ref[...] = (part_ref[...].astype(jnp.float32) + rest).astype(jnp.bfloat16)

    return pl.pallas_call(
        kernel,
        out_shape=jax.ShapeDtypeStruct(part.shape, jnp.bfloat16),
        in_specs=[SMEM, VMEM, VMEM, VMEM],
        out_specs=VMEM,
        compiler_params=limit(16),
        name="embed",
    )(core, ids, part, other)


def squares_of(side, embedded, weights, groups):
    columns = weights.shape[0] // groups
    tasks = embedded.shape[0] // 2
    chunks = tasks // LANES

    def kernel(side_ref, embedded_ref, weights_ref, squares_ref):
        wanted = embedded_ref[pl.ds(pl.multiple_of(side_ref[0] * tasks, tasks), tasks), :]
        for g in range(groups):
            made = lax.dot_general(
                weights_ref[g * columns : (g + 1) * columns, :],
                wanted,
                ROWS_BY_ROWS,
                preferred_element_type=jnp.float32,
            )
            total = jnp.sum(made * made, axis=0, keepdims=True)
            for k in range(chunks):
                squares_ref[k, g : g + 1, :] = total[:, k * LANES : (k + 1) * LANES]

    return pl.pallas_call(
        kernel,
        out_shape=jax.ShapeDtypeStruct((chunks, groups, LANES), jnp.float32),
        in_specs=[SMEM, VMEM, VMEM],
        out_specs=VMEM,
        compiler_params=limit(16),
        name="squares",
    )(side, embedded, weights)


def split_by_row(row, keep, received):
    count = keep.shape[0]

    def kernel(row_ref, keep_ref, received_ref, *out_refs):
        for ahead, out_ref in enumerate(out_refs):
            chunk = lax.rem(row_ref[0] + ahead, count)
            out_ref[...] = keep_ref[chunk] + received_ref[chunk]

    return pl.pallas_call(
        kernel,
        out_shape=[jax.ShapeDtypeStruct(keep.shape[1:], jnp.float32)] * count,
        in_specs=[SMEM, VMEM, VMEM],
        out_specs=[VMEM] * count,
        compiler_params=limit(4),
        name="split_by_row",
    )(row, keep, received)


def sum_for_each(pieces, copies):
    def kernel(*refs):
        total = refs[0][...]
        for piece_ref in refs[1:-1]:
            total = total + piece_ref[...]
        for copy in range(copies):
            refs[-1][copy] = total

    return pl.pallas_call(
        kernel,
        out_shape=jax.ShapeDtypeStruct((copies, *pieces[0].shape), jnp.float32),
        in_specs=[VMEM] * len(pieces),
        out_specs=VMEM,
        compiler_params=limit(4),
        name="sum_for_each",
    )(*pieces)


def around(x, axis, ahead):
    size = lax.axis_size(axis)
    return lax.ppermute(x, axis, [(i, (i + ahead) % size) for i in range(size)])


def scaled_adapters(core, row, weights, embedded, pairs, gain):
    rows_of_chips = len(pairs)
    groups, columns = gain.shape
    tasks, width = embedded.shape
    padding = -columns % LANES

    def kernel(core_ref, row_ref, weights_ref, embedded_ref, *refs):
        pair_refs, (gain_ref, out_hbm, out_ref, totals_ref, sems) = refs[:rows_of_chips], refs[rows_of_chips:]
        for behind in range(rows_of_chips):
            chunk = lax.rem(row_ref[0] + rows_of_chips - behind, rows_of_chips)
            totals_ref[core_ref[0] * rows_of_chips + chunk] = pair_refs[behind][0]
            totals_ref[(1 - core_ref[0]) * rows_of_chips + chunk] = pair_refs[behind][1]
        gains = gain_ref[...].astype(jnp.float32)
        gains = jnp.transpose(jnp.concatenate([gains, jnp.zeros((groups, padding), jnp.float32)], axis=1))
        stores = []
        for g in range(groups):
            rows = pl.ds(g * columns, columns)
            power = jnp.concatenate([totals_ref[k, g : g + 1, :] for k in range(2 * rows_of_chips)], axis=1)
            inverse = lax.rsqrt(power / BLOCK + EPSILON)
            made = lax.dot_general(
                weights_ref[g * columns : (g + 1) * columns, :],
                embedded_ref[...],
                ROWS_BY_ROWS,
                preferred_element_type=jnp.float32,
            )
            out_ref[g] = (made * inverse * gains[:columns, g : g + 1]).astype(jnp.bfloat16)
            store = pltpu.make_async_copy(out_ref.at[g], out_hbm.at[rows, :], sems.at[g])
            store.start()
            stores.append(store)
        for store in stores:
            store.wait()

    return pl.pallas_call(
        kernel,
        out_shape=jax.ShapeDtypeStruct((groups * columns, tasks), jnp.bfloat16),
        in_specs=[SMEM, SMEM] + [VMEM] * (3 + len(pairs)),
        out_specs=HBM,
        scratch_shapes=[
            pltpu.VMEM((groups, columns, tasks), jnp.bfloat16),
            pltpu.VMEM((2 * rows_of_chips, groups, LANES), jnp.float32),
            pltpu.SemaphoreType.DMA((groups,)),
        ],
        compiler_params=limit(24),
        name="scale",
    )(core, row, weights, embedded, *pairs, gain)


def on_device(task_ids, task_table, enc_in, enc_out, generator, gain):
    width, groups, columns = generator.shape
    half = task_table.shape[0] // 2
    core = lax.axis_index("core").reshape(1).astype(jnp.int32)
    row = lax.axis_index("y").reshape(1).astype(jnp.int32)
    weights = generator.transpose(1, 2, 0).reshape(groups * columns, width)
    copies = encode_half(core, task_table, enc_in, enc_out, lax.axis_size(PARAM))
    task_ids, copies = lax.optimization_barrier((task_ids, copies))
    mine = exchange(copies, PARAM).reshape(-1, width)
    ids = lax.all_gather(task_ids.reshape(1, -1), TASK, axis=0, tiled=True)
    mine, ids = lax.optimization_barrier((mine, ids))
    other = lax.ppermute(mine, "core", [(0, 1), (1, 0)])
    part, weights = first_half(core, ids, mine, weights, half)
    embedded = embed(core, ids, part, other, half)
    given = squares_of(1 - core, embedded, weights, groups)
    received = around(given, "core", 1)
    kept = squares_of(core, embedded, weights, groups)
    own, *others = split_by_row(row, kept, received)
    steps = range(1, len(others) + 1)
    arrived = [around(piece, "y", ahead) for ahead, piece in zip(steps, others)]
    totals = exchange(sum_for_each([own, *arrived], lax.axis_size(PARAM)), PARAM).sum(axis=0)
    pair = jnp.stack([totals, around(totals, "core", 1)])
    pairs = [pair] + [around(pair, "y", ahead) for ahead in steps]
    made = scaled_adapters(core, row, weights, embedded, pairs, gain)
    return made.reshape(groups, columns, -1).transpose(2, 0, 1)


def solution(mesh):
    torus = Mesh(mesh.devices.reshape(8, 4, 4, 2), PARAM_TASK)
    return jax.shard_map(
        on_device,
        mesh=torus,
        in_specs=(
            P(TASK),
            P(PARAM, None),
            P(),
            P(),
            P(None, None, PARAM_TASK),
            P(None, PARAM_TASK),
        ),
        out_specs=P(None, None, PARAM_TASK),
        check_vma=False,
    )
```

```python
import jax
import jax.numpy as jnp
from jax import lax
from jax.experimental import pallas as pl
from jax.experimental.pallas import tpu as pltpu
from jax.sharding import Mesh
from jax.sharding import PartitionSpec as P

BLOCK = 114688
PARAM = ("z", "x")
TASK = ("y", "core")
PARAM_TASK = ("z", "x", "y", "core")
PLANE = ("x", "y")
COLUMN = "z"
LANES = 128
EPSILON = 1e-06

VMEM = pl.BlockSpec(memory_space=pltpu.VMEM)
HBM = pl.BlockSpec(memory_space=pltpu.HBM)
SMEM = pl.BlockSpec(memory_space=pltpu.SMEM)
ROWS_BY_ROWS = (((1,), (1,)), ((), ()))


def in_hbm(x):
    return pltpu.with_memory_space_constraint(x, pltpu.HBM)


def limit(mebibytes):
    return pltpu.CompilerParams(vmem_limit_bytes=mebibytes << 20)


def exchange(x, axis):
    return lax.all_to_all(x, axis, split_axis=0, concat_axis=0, tiled=True)


def copy_for_each(x, axis):
    return exchange(jnp.broadcast_to(x, (lax.axis_size(axis), *x.shape)), axis)


def encode_kernel(core_ref, table_hbm, enc_in_hbm, enc_out_hbm, out_ref, table_ref, enc_in_ref, enc_out_ref, sems):
    copies, rows, _ = out_ref.shape
    start = pl.multiple_of(core_ref[0] * rows, rows)
    loads = [
        pltpu.make_async_copy(table_hbm.at[pl.ds(start, rows), :], table_ref, sems.at[0]),
        pltpu.make_async_copy(enc_in_hbm, enc_in_ref, sems.at[1]),
        pltpu.make_async_copy(enc_out_hbm, enc_out_ref, sems.at[2]),
    ]
    for load in loads:
        load.start()
    loads[0].wait()
    loads[1].wait()
    raw = table_ref[...]
    inner = jax.nn.gelu(jnp.dot(raw, enc_in_ref[...], preferred_element_type=jnp.float32)).astype(jnp.bfloat16)
    loads[2].wait()
    mixed = raw.astype(jnp.float32) + jnp.dot(inner, enc_out_ref[...], preferred_element_type=jnp.float32)
    encoded = mixed.astype(jnp.bfloat16)
    for copy in range(copies):
        out_ref[copy] = encoded


def encode_half(core, task_table, enc_in, enc_out, copies):
    rows, width = task_table.shape[0] // 2, task_table.shape[1]
    return pl.pallas_call(
        encode_kernel,
        out_shape=jax.ShapeDtypeStruct((copies, rows, width), jnp.bfloat16),
        in_specs=[SMEM, HBM, HBM, HBM],
        out_specs=VMEM,
        scratch_shapes=[
            pltpu.VMEM((rows, width), jnp.bfloat16),
            pltpu.VMEM(enc_in.shape, jnp.bfloat16),
            pltpu.VMEM(enc_out.shape, jnp.bfloat16),
            pltpu.SemaphoreType.DMA((3,)),
        ],
        compiler_params=limit(8),
        name="encode_half",
    )(core, in_hbm(task_table), in_hbm(enc_in), in_hbm(enc_out))


def picked_rows(ids_ref, part_ref, which, half):
    chunks = ids_ref.shape[0]
    ids = jnp.transpose(ids_ref[...])
    place = lax.broadcasted_iota(jnp.int32, (1, part_ref.shape[0]), 1)
    labels = (place // half) * (2 * half) + place % half + which * half
    hot = [(ids[:, k : k + 1] == labels).astype(jnp.bfloat16) for k in range(chunks)]
    return jnp.dot(jnp.concatenate(hot, axis=0), part_ref[...], preferred_element_type=jnp.float32)


def first_half(core, ids, mine, weights, half):
    def kernel(core_ref, ids_ref, mine_ref, weights_hbm, part_ref, weights_ref, sem):
        load = pltpu.make_async_copy(weights_hbm, weights_ref, sem)
        load.start()
        part_ref[...] = picked_rows(ids_ref, mine_ref, core_ref[0], half).astype(jnp.bfloat16)
        load.wait()

    return pl.pallas_call(
        kernel,
        out_shape=(
            jax.ShapeDtypeStruct((ids.size, mine.shape[1]), jnp.bfloat16),
            jax.ShapeDtypeStruct(weights.shape, weights.dtype),
        ),
        in_specs=[SMEM, VMEM, VMEM, HBM],
        out_specs=(VMEM, VMEM),
        scratch_shapes=[pltpu.SemaphoreType.DMA],
        compiler_params=limit(16),
        name="first_half",
    )(core, ids, mine, in_hbm(weights))


def embed(core, ids, part, other, half):
    def kernel(core_ref, ids_ref, part_ref, other_ref, embedded_ref):
        rest = picked_rows(ids_ref, other_ref, 1 - core_ref[0], half)
        embedded_ref[...] = (part_ref[...].astype(jnp.float32) + rest).astype(jnp.bfloat16)

    return pl.pallas_call(
        kernel,
        out_shape=jax.ShapeDtypeStruct(part.shape, jnp.bfloat16),
        in_specs=[SMEM, VMEM, VMEM, VMEM],
        out_specs=VMEM,
        compiler_params=limit(16),
        name="embed",
    )(core, ids, part, other)


def squares_of(side, embedded, weights, groups):
    columns = weights.shape[0] // groups
    tasks = embedded.shape[0] // 2
    chunks = tasks // LANES

    def kernel(side_ref, embedded_ref, weights_ref, squares_ref):
        wanted = embedded_ref[pl.ds(pl.multiple_of(side_ref[0] * tasks, tasks), tasks), :]
        for g in range(groups):
            made = lax.dot_general(
                weights_ref[g * columns : (g + 1) * columns, :],
                wanted,
                ROWS_BY_ROWS,
                preferred_element_type=jnp.float32,
            )
            total = jnp.sum(made * made, axis=0, keepdims=True)
            for k in range(chunks):
                squares_ref[k, g : g + 1, :] = total[:, k * LANES : (k + 1) * LANES]

    return pl.pallas_call(
        kernel,
        out_shape=jax.ShapeDtypeStruct((chunks, groups, LANES), jnp.float32),
        in_specs=[SMEM, VMEM, VMEM],
        out_specs=VMEM,
        compiler_params=limit(16),
        name="squares",
    )(side, embedded, weights)


def sum_for_each(pieces, copies):
    def kernel(pieces_ref, out_ref):
        total = pieces_ref[0]
        for i in range(1, pieces_ref.shape[0]):
            total = total + pieces_ref[i]
        for copy in range(copies):
            out_ref[copy] = total

    return pl.pallas_call(
        kernel,
        out_shape=jax.ShapeDtypeStruct((copies, *pieces.shape[1:]), jnp.float32),
        in_specs=[VMEM],
        out_specs=VMEM,
        compiler_params=limit(8),
        name="sum_for_each",
    )(pieces)


def pair_for_each(kept, received, copies):
    def kernel(kept_ref, received_ref, out_ref):
        total = kept_ref[...] + received_ref[...]
        for copy in range(copies):
            out_ref[copy] = total

    return pl.pallas_call(
        kernel,
        out_shape=jax.ShapeDtypeStruct((copies, *kept.shape), jnp.float32),
        in_specs=[VMEM, VMEM],
        out_specs=VMEM,
        compiler_params=limit(8),
        name="pair_for_each",
    )(kept, received)


def around(x, axis, ahead):
    size = lax.axis_size(axis)
    return lax.ppermute(x, axis, [(i, (i + ahead) % size) for i in range(size)])


def scaled_adapters(side, weights, embedded, totals, gain, before=None):
    groups, columns = gain.shape
    chunks = totals.shape[0]
    tasks = chunks * LANES
    padding = -columns % LANES

    def kernel(side_ref, weights_ref, embedded_ref, totals_ref, gain_ref, *refs):
        out_hbm, out_ref, sems = refs[-3:]
        start = pl.multiple_of(side_ref[0] * tasks, tasks)
        wanted = embedded_ref[pl.ds(start, tasks), :]
        gains = gain_ref[...].astype(jnp.float32)
        gains = jnp.transpose(jnp.concatenate([gains, jnp.zeros((groups, padding), jnp.float32)], axis=1))
        stores = []
        for g in range(groups):
            power = jnp.concatenate([totals_ref[k, g : g + 1, :] for k in range(chunks)], axis=1)
            inverse = lax.rsqrt(power / BLOCK + EPSILON)
            made = lax.dot_general(
                weights_ref[g * columns : (g + 1) * columns, :],
                wanted,
                ROWS_BY_ROWS,
                preferred_element_type=jnp.float32,
            )
            out_ref[g] = (made * inverse * gains[:columns, g : g + 1]).astype(jnp.bfloat16)
            place = out_hbm.at[pl.ds(g * columns, columns), pl.ds(start, tasks)]
            store = pltpu.make_async_copy(out_ref.at[g], place, sems.at[g])
            store.start()
            stores.append(store)
        for store in stores:
            store.wait()

    operands = [side, weights, embedded, totals, gain]
    specs = [SMEM, VMEM, VMEM, VMEM, VMEM]
    aliases = {}
    if before is not None:
        aliases = {len(operands): 0}
        operands.append(before)
        specs.append(HBM)
    return pl.pallas_call(
        kernel,
        out_shape=jax.ShapeDtypeStruct((groups * columns, embedded.shape[0]), jnp.bfloat16),
        in_specs=specs,
        out_specs=HBM,
        scratch_shapes=[pltpu.VMEM((groups, columns, tasks), jnp.bfloat16), pltpu.SemaphoreType.DMA((groups,))],
        input_output_aliases=aliases,
        compiler_params=limit(16),
        name="scale",
    )(*operands)


def on_device(task_ids, task_table, enc_in, enc_out, generator, gain):
    width, groups, columns = generator.shape
    half = task_table.shape[0] // 2
    core = lax.axis_index("core").reshape(1).astype(jnp.int32)
    weights = generator.transpose(1, 2, 0).reshape(groups * columns, width)
    copies = encode_half(core, task_table, enc_in, enc_out, lax.axis_size(PARAM))
    task_ids, copies = lax.optimization_barrier((task_ids, copies))
    mine = exchange(copies, PARAM).reshape(-1, width)
    ids = lax.all_gather(task_ids.reshape(1, -1), TASK, axis=0, tiled=True)
    mine, ids = lax.optimization_barrier((mine, ids))
    other = lax.ppermute(mine, "core", [(0, 1), (1, 0)])
    part, weights = first_half(core, ids, mine, weights, half)
    embedded = embed(core, ids, part, other, half)
    given = squares_of(1 - core, embedded, weights, groups)
    received = around(given, "core", 1)
    kept = squares_of(core, embedded, weights, groups)
    plane = exchange(pair_for_each(kept, received, lax.axis_size(PLANE)), PLANE)
    column = exchange(sum_for_each(plane, lax.axis_size(COLUMN)), COLUMN)
    totals = sum_for_each(column, 1)[0]
    others = around(totals, "core", 1)
    made = scaled_adapters(core, weights, embedded, totals, gain)
    made = scaled_adapters(1 - core, weights, embedded, others, gain, made)
    return made.reshape(groups, columns, -1).transpose(2, 0, 1)


def solution(mesh):
    torus = Mesh(mesh.devices.reshape(8, 4, 4, 2), PARAM_TASK)
    return jax.shard_map(
        on_device,
        mesh=torus,
        in_specs=(
            P(TASK),
            P(PARAM, None),
            P(),
            P(),
            P(None, None, PARAM_TASK),
            P(None, PARAM_TASK),
        ),
        out_specs=P(None, None, PARAM_TASK),
        check_vma=False,
    )
```

```python
import jax
import jax.numpy as jnp
from jax import lax
from jax.experimental import pallas as pl
from jax.experimental.pallas import tpu as pltpu
from jax.sharding import Mesh
from jax.sharding import PartitionSpec as P

BLOCK = 114688
PARAM = ("z", "x")
TASK = ("y", "core")
PARAM_TASK = ("z", "x", "y", "core")
PLANE = ("x", "y")
COLUMN = "z"
LANES = 128
QUARTERS = 4
EPSILON = 1e-06

VMEM = pl.BlockSpec(memory_space=pltpu.VMEM)
HBM = pl.BlockSpec(memory_space=pltpu.HBM)
SMEM = pl.BlockSpec(memory_space=pltpu.SMEM)
ROWS_BY_ROWS = (((1,), (1,)), ((), ()))


def in_hbm(x):
    return pltpu.with_memory_space_constraint(x, pltpu.HBM)


def limit(mebibytes):
    return pltpu.CompilerParams(vmem_limit_bytes=mebibytes << 20)


def exchange(x, axis):
    return lax.all_to_all(x, axis, split_axis=0, concat_axis=0, tiled=True)


def copy_for_each(x, axis):
    return exchange(jnp.broadcast_to(x, (lax.axis_size(axis), *x.shape)), axis)


def encode_kernel(slot_ref, table_hbm, enc_in_hbm, enc_out_hbm, out_ref, table_ref, enc_in_ref, enc_out_ref, sems):
    copies, rows, _ = out_ref.shape
    start = pl.multiple_of(slot_ref[0] * rows, rows)
    loads = [
        pltpu.make_async_copy(table_hbm.at[pl.ds(start, rows), :], table_ref, sems.at[0]),
        pltpu.make_async_copy(enc_in_hbm, enc_in_ref, sems.at[1]),
        pltpu.make_async_copy(enc_out_hbm, enc_out_ref, sems.at[2]),
    ]
    for load in loads:
        load.start()
    loads[0].wait()
    loads[1].wait()
    raw = table_ref[...]
    inner = jax.nn.gelu(jnp.dot(raw, enc_in_ref[...], preferred_element_type=jnp.float32)).astype(jnp.bfloat16)
    loads[2].wait()
    mixed = raw.astype(jnp.float32) + jnp.dot(inner, enc_out_ref[...], preferred_element_type=jnp.float32)
    encoded = mixed.astype(jnp.bfloat16)
    for copy in range(copies):
        out_ref[copy] = encoded


def encode_quarter(slot, task_table, enc_in, enc_out, copies):
    rows, width = task_table.shape[0] // QUARTERS, task_table.shape[1]
    return pl.pallas_call(
        encode_kernel,
        out_shape=jax.ShapeDtypeStruct((copies, rows, width), jnp.bfloat16),
        in_specs=[SMEM, HBM, HBM, HBM],
        out_specs=VMEM,
        scratch_shapes=[
            pltpu.VMEM((rows, width), jnp.bfloat16),
            pltpu.VMEM(enc_in.shape, jnp.bfloat16),
            pltpu.VMEM(enc_out.shape, jnp.bfloat16),
            pltpu.SemaphoreType.DMA((3,)),
        ],
        compiler_params=limit(8),
        name="encode_quarter",
    )(slot, in_hbm(task_table), in_hbm(enc_in), in_hbm(enc_out))


def split_in_two(x):
    size = x.shape[0] // 2

    def kernel(x_ref, low_ref, high_ref):
        low_ref[...] = x_ref[:size]
        high_ref[...] = x_ref[size:]

    return pl.pallas_call(
        kernel,
        out_shape=[jax.ShapeDtypeStruct((size, *x.shape[1:]), x.dtype)] * 2,
        in_specs=[VMEM],
        out_specs=[VMEM, VMEM],
        compiler_params=limit(4),
        name="split_in_two",
    )(x)


def joined(low, high):
    size = low.shape[0]

    def kernel(low_ref, high_ref, out_ref):
        out_ref[:size] = low_ref[...]
        out_ref[size:] = high_ref[...]

    return pl.pallas_call(
        kernel,
        out_shape=jax.ShapeDtypeStruct((2 * size, *low.shape[1:]), low.dtype),
        in_specs=[VMEM, VMEM],
        out_specs=VMEM,
        compiler_params=limit(4),
        name="joined",
    )(low, high)


def picked_rows(slot_ref, ids_ref, rows_ref, size):
    chunks = ids_ref.shape[0]
    ids = jnp.transpose(ids_ref[...])
    place = lax.broadcasted_iota(jnp.int32, (1, rows_ref.shape[0]), 1)
    labels = (place // size) * (QUARTERS * size) + place % size + slot_ref[0] * size
    hot = [(ids[:, k : k + 1] == labels).astype(jnp.bfloat16) for k in range(chunks)]
    return jnp.dot(jnp.concatenate(hot, axis=0), rows_ref[...], preferred_element_type=jnp.float32)


def pick_first(slot, ids, rows, weights, size):
    def kernel(slot_ref, ids_ref, rows_ref, weights_hbm, part_ref, weights_ref, sem):
        load = pltpu.make_async_copy(weights_hbm, weights_ref, sem)
        load.start()
        part_ref[...] = picked_rows(slot_ref, ids_ref, rows_ref, size).astype(jnp.bfloat16)
        load.wait()

    return pl.pallas_call(
        kernel,
        out_shape=(
            jax.ShapeDtypeStruct((ids.size, rows.shape[1]), jnp.bfloat16),
            jax.ShapeDtypeStruct(weights.shape, weights.dtype),
        ),
        in_specs=[SMEM, VMEM, VMEM, HBM],
        out_specs=(VMEM, VMEM),
        scratch_shapes=[pltpu.SemaphoreType.DMA],
        compiler_params=limit(16),
        name="pick_first",
    )(slot, ids, rows, in_hbm(weights))


def pick_more(slot, ids, rows, part, size):
    def kernel(slot_ref, ids_ref, rows_ref, part_ref, out_ref):
        more = picked_rows(slot_ref, ids_ref, rows_ref, size)
        out_ref[...] = (part_ref[...].astype(jnp.float32) + more).astype(jnp.bfloat16)

    return pl.pallas_call(
        kernel,
        out_shape=jax.ShapeDtypeStruct(part.shape, jnp.bfloat16),
        in_specs=[SMEM, VMEM, VMEM, VMEM],
        out_specs=VMEM,
        compiler_params=limit(16),
        name="pick_more",
    )(slot, ids, rows, part)


def squares_of(side, embedded, weights, groups):
    columns = weights.shape[0] // groups
    tasks = embedded.shape[0] // 2
    chunks = tasks // LANES

    def kernel(side_ref, embedded_ref, weights_ref, squares_ref):
        wanted = embedded_ref[pl.ds(pl.multiple_of(side_ref[0] * tasks, tasks), tasks), :]
        for g in range(groups):
            made = lax.dot_general(
                weights_ref[g * columns : (g + 1) * columns, :],
                wanted,
                ROWS_BY_ROWS,
                preferred_element_type=jnp.float32,
            )
            total = jnp.sum(made * made, axis=0, keepdims=True)
            for k in range(chunks):
                squares_ref[k, g : g + 1, :] = total[:, k * LANES : (k + 1) * LANES]

    return pl.pallas_call(
        kernel,
        out_shape=jax.ShapeDtypeStruct((chunks, groups, LANES), jnp.float32),
        in_specs=[SMEM, VMEM, VMEM],
        out_specs=VMEM,
        compiler_params=limit(16),
        name="squares",
    )(side, embedded, weights)


def sum_for_each(pieces, copies):
    def kernel(pieces_ref, out_ref):
        total = pieces_ref[0]
        for i in range(1, pieces_ref.shape[0]):
            total = total + pieces_ref[i]
        for copy in range(copies):
            out_ref[copy] = total

    return pl.pallas_call(
        kernel,
        out_shape=jax.ShapeDtypeStruct((copies, *pieces.shape[1:]), jnp.float32),
        in_specs=[VMEM],
        out_specs=VMEM,
        compiler_params=limit(8),
        name="sum_for_each",
    )(pieces)


def pair_for_each(kept, received, copies):
    def kernel(kept_ref, received_ref, out_ref):
        total = kept_ref[...] + received_ref[...]
        for copy in range(copies):
            out_ref[copy] = total

    return pl.pallas_call(
        kernel,
        out_shape=jax.ShapeDtypeStruct((copies, *kept.shape), jnp.float32),
        in_specs=[VMEM, VMEM],
        out_specs=VMEM,
        compiler_params=limit(8),
        name="pair_for_each",
    )(kept, received)


def around(x, axis, ahead):
    size = lax.axis_size(axis)
    return lax.ppermute(x, axis, [(i, (i + ahead) % size) for i in range(size)])


def scaled_adapters(side, weights, embedded, totals, gain, before=None):
    groups, columns = gain.shape
    chunks = totals.shape[0]
    tasks = chunks * LANES
    padding = -columns % LANES

    def kernel(side_ref, weights_ref, embedded_ref, totals_ref, gain_ref, *refs):
        out_hbm, out_ref, sems = refs[-3:]
        start = pl.multiple_of(side_ref[0] * tasks, tasks)
        wanted = embedded_ref[pl.ds(start, tasks), :]
        gains = gain_ref[...].astype(jnp.float32)
        gains = jnp.transpose(jnp.concatenate([gains, jnp.zeros((groups, padding), jnp.float32)], axis=1))
        stores = []
        for g in range(groups):
            power = jnp.concatenate([totals_ref[k, g : g + 1, :] for k in range(chunks)], axis=1)
            inverse = lax.rsqrt(power / BLOCK + EPSILON)
            made = lax.dot_general(
                weights_ref[g * columns : (g + 1) * columns, :],
                wanted,
                ROWS_BY_ROWS,
                preferred_element_type=jnp.float32,
            )
            out_ref[g] = (made * inverse * gains[:columns, g : g + 1]).astype(jnp.bfloat16)
            place = out_hbm.at[pl.ds(g * columns, columns), pl.ds(start, tasks)]
            store = pltpu.make_async_copy(out_ref.at[g], place, sems.at[g])
            store.start()
            stores.append(store)
        for store in stores:
            store.wait()

    operands = [side, weights, embedded, totals, gain]
    specs = [SMEM, VMEM, VMEM, VMEM, VMEM]
    aliases = {}
    if before is not None:
        aliases = {len(operands): 0}
        operands.append(before)
        specs.append(HBM)
    return pl.pallas_call(
        kernel,
        out_shape=jax.ShapeDtypeStruct((groups * columns, embedded.shape[0]), jnp.bfloat16),
        in_specs=specs,
        out_specs=HBM,
        scratch_shapes=[pltpu.VMEM((groups, columns, tasks), jnp.bfloat16), pltpu.SemaphoreType.DMA((groups,))],
        input_output_aliases=aliases,
        compiler_params=limit(16),
        name="scale",
    )(*operands)


def on_device(task_ids, task_table, enc_in, enc_out, generator, gain):
    width, groups, columns = generator.shape
    size = task_table.shape[0] // QUARTERS
    core = lax.axis_index("core").reshape(1).astype(jnp.int32)
    parity = lax.axis_index("y").reshape(1).astype(jnp.int32) & 1
    weights = generator.transpose(1, 2, 0).reshape(groups * columns, width)
    copies = encode_quarter(2 * core + parity, task_table, enc_in, enc_out, lax.axis_size(PARAM))
    task_ids, copies = lax.optimization_barrier((task_ids, copies))
    mine = exchange(copies, PARAM).reshape(-1, width)
    ids = lax.all_gather(task_ids.reshape(1, -1), TASK, axis=0, tiled=True)
    mine, ids = lax.optimization_barrier((mine, ids))
    low, high = split_in_two(mine)
    low, high = around(low, "y", 1), around(high, "y", -1)
    swapped = around(mine, "core", 1)
    part, weights = pick_first(2 * core + parity, ids, mine, weights, size)
    part = pick_more(2 * (1 - core) + parity, ids, swapped, part, size)
    low, high, part = lax.optimization_barrier((low, high, part))
    beside = joined(low, high)
    far = around(beside, "core", 1)
    part = pick_more(2 * core + 1 - parity, ids, beside, part, size)
    embedded = pick_more(2 * (1 - core) + 1 - parity, ids, far, part, size)
    given = squares_of(1 - core, embedded, weights, groups)
    received = around(given, "core", 1)
    kept = squares_of(core, embedded, weights, groups)
    plane = exchange(pair_for_each(kept, received, lax.axis_size(PLANE)), PLANE)
    column = exchange(sum_for_each(plane, lax.axis_size(COLUMN)), COLUMN)
    totals = sum_for_each(column, 1)[0]
    others = around(totals, "core", 1)
    made = scaled_adapters(core, weights, embedded, totals, gain)
    made = scaled_adapters(1 - core, weights, embedded, others, gain, made)
    return made.reshape(groups, columns, -1).transpose(2, 0, 1)


def solution(mesh):
    torus = Mesh(mesh.devices.reshape(8, 4, 4, 2), PARAM_TASK)
    return jax.shard_map(
        on_device,
        mesh=torus,
        in_specs=(
            P(TASK),
            P(PARAM, None),
            P(),
            P(),
            P(None, None, PARAM_TASK),
            P(None, PARAM_TASK),
        ),
        out_specs=P(None, None, PARAM_TASK),
        check_vma=False,
    )
```

```python
import jax
import jax.numpy as jnp
from jax import lax
from jax.experimental import pallas as pl
from jax.experimental.pallas import tpu as pltpu
from jax.sharding import Mesh
from jax.sharding import PartitionSpec as P

BLOCK = 114688
PARAM = ("z", "x")
TASK = ("y", "core")
PARAM_TASK = ("z", "x", "y", "core")
PLANE = ("x", "y")
COLUMN = "z"
LANES = 128
EPSILON = 1e-06

VMEM = pl.BlockSpec(memory_space=pltpu.VMEM)
HBM = pl.BlockSpec(memory_space=pltpu.HBM)
SMEM = pl.BlockSpec(memory_space=pltpu.SMEM)
ROWS_BY_ROWS = (((1,), (1,)), ((), ()))


def in_hbm(x):
    return pltpu.with_memory_space_constraint(x, pltpu.HBM)


def limit(mebibytes):
    return pltpu.CompilerParams(vmem_limit_bytes=mebibytes << 20)


def exchange(x, axis):
    return lax.all_to_all(x, axis, split_axis=0, concat_axis=0, tiled=True)


def copy_for_each(x, axis):
    return exchange(jnp.broadcast_to(x, (lax.axis_size(axis), *x.shape)), axis)


def encode_kernel(core_ref, table_hbm, enc_in_hbm, enc_out_hbm, out_ref, table_ref, enc_in_ref, enc_out_ref, sems):
    copies, rows, _ = out_ref.shape
    start = pl.multiple_of(core_ref[0] * rows, rows)
    loads = [
        pltpu.make_async_copy(table_hbm.at[pl.ds(start, rows), :], table_ref, sems.at[0]),
        pltpu.make_async_copy(enc_in_hbm, enc_in_ref, sems.at[1]),
        pltpu.make_async_copy(enc_out_hbm, enc_out_ref, sems.at[2]),
    ]
    for load in loads:
        load.start()
    loads[0].wait()
    loads[1].wait()
    raw = table_ref[...]
    inner = jax.nn.gelu(jnp.dot(raw, enc_in_ref[...], preferred_element_type=jnp.float32)).astype(jnp.bfloat16)
    loads[2].wait()
    mixed = raw.astype(jnp.float32) + jnp.dot(inner, enc_out_ref[...], preferred_element_type=jnp.float32)
    encoded = mixed.astype(jnp.bfloat16)
    for copy in range(copies):
        out_ref[copy] = encoded


def encode_half(core, task_table, enc_in, enc_out, copies):
    rows, width = task_table.shape[0] // 2, task_table.shape[1]
    return pl.pallas_call(
        encode_kernel,
        out_shape=jax.ShapeDtypeStruct((copies, rows, width), jnp.bfloat16),
        in_specs=[SMEM, HBM, HBM, HBM],
        out_specs=VMEM,
        scratch_shapes=[
            pltpu.VMEM((rows, width), jnp.bfloat16),
            pltpu.VMEM(enc_in.shape, jnp.bfloat16),
            pltpu.VMEM(enc_out.shape, jnp.bfloat16),
            pltpu.SemaphoreType.DMA((3,)),
        ],
        compiler_params=limit(8),
        name="encode_half",
    )(core, in_hbm(task_table), in_hbm(enc_in), in_hbm(enc_out))


def loaded(weights, after):
    def kernel(weights_hbm, after_ref, out_ref, sem):
        load = pltpu.make_async_copy(weights_hbm, out_ref, sem)
        load.start()
        load.wait()

    return pl.pallas_call(
        kernel,
        out_shape=jax.ShapeDtypeStruct(weights.shape, weights.dtype),
        in_specs=[HBM, VMEM],
        out_specs=VMEM,
        scratch_shapes=[pltpu.SemaphoreType.DMA],
        compiler_params=limit(8),
        name="loaded",
    )(in_hbm(weights), after)


def split_in_two(x):
    size = x.shape[0] // 2

    def kernel(x_ref, low_ref, high_ref):
        low_ref[...] = x_ref[:size]
        high_ref[...] = x_ref[size:]

    return pl.pallas_call(
        kernel,
        out_shape=[jax.ShapeDtypeStruct((size, *x.shape[1:]), x.dtype)] * 2,
        in_specs=[VMEM],
        out_specs=[VMEM, VMEM],
        compiler_params=limit(4),
        name="split_in_two",
    )(x)


def picked(core, ids, rows, half, offset=0, part=None):
    chunks = ids.shape[0]

    def kernel(core_ref, ids_ref, rows_ref, *refs):
        turned = jnp.transpose(ids_ref[...])
        place = offset + lax.broadcasted_iota(jnp.int32, (1, rows_ref.shape[0]), 1)
        labels = (place // half) * (2 * half) + place % half + core_ref[0] * half
        hot = [(turned[:, k : k + 1] == labels).astype(jnp.bfloat16) for k in range(chunks)]
        found = jnp.dot(jnp.concatenate(hot, axis=0), rows_ref[...], preferred_element_type=jnp.float32)
        if part is not None:
            found = found + refs[0][...].astype(jnp.float32)
        refs[-1][...] = found.astype(jnp.bfloat16)

    operands = [core, ids, rows] + ([] if part is None else [part])
    return pl.pallas_call(
        kernel,
        out_shape=jax.ShapeDtypeStruct((ids.size, rows.shape[1]), jnp.bfloat16),
        in_specs=[SMEM] + [VMEM] * (len(operands) - 1),
        out_specs=VMEM,
        compiler_params=limit(16),
        name="picked",
    )(*operands)


def squares_of(side, embedded, weights, groups):
    columns = weights.shape[0] // groups
    tasks = embedded.shape[0] // 2
    chunks = tasks // LANES

    def kernel(side_ref, embedded_ref, weights_ref, squares_ref):
        wanted = embedded_ref[pl.ds(pl.multiple_of(side_ref[0] * tasks, tasks), tasks), :]
        for g in range(groups):
            made = lax.dot_general(
                weights_ref[g * columns : (g + 1) * columns, :],
                wanted,
                ROWS_BY_ROWS,
                preferred_element_type=jnp.float32,
            )
            total = jnp.sum(made * made, axis=0, keepdims=True)
            for k in range(chunks):
                squares_ref[k, g : g + 1, :] = total[:, k * LANES : (k + 1) * LANES]

    return pl.pallas_call(
        kernel,
        out_shape=jax.ShapeDtypeStruct((chunks, groups, LANES), jnp.float32),
        in_specs=[SMEM, VMEM, VMEM],
        out_specs=VMEM,
        compiler_params=limit(16),
        name="squares",
    )(side, embedded, weights)


def sum_for_each(pieces, copies):
    def kernel(pieces_ref, out_ref):
        total = pieces_ref[0]
        for i in range(1, pieces_ref.shape[0]):
            total = total + pieces_ref[i]
        for copy in range(copies):
            out_ref[copy] = total

    return pl.pallas_call(
        kernel,
        out_shape=jax.ShapeDtypeStruct((copies, *pieces.shape[1:]), jnp.float32),
        in_specs=[VMEM],
        out_specs=VMEM,
        compiler_params=limit(8),
        name="sum_for_each",
    )(pieces)


def pair_for_each(kept, received, copies):
    def kernel(kept_ref, received_ref, out_ref):
        total = kept_ref[...] + received_ref[...]
        for copy in range(copies):
            out_ref[copy] = total

    return pl.pallas_call(
        kernel,
        out_shape=jax.ShapeDtypeStruct((copies, *kept.shape), jnp.float32),
        in_specs=[VMEM, VMEM],
        out_specs=VMEM,
        compiler_params=limit(8),
        name="pair_for_each",
    )(kept, received)


def around(x, axis, ahead):
    size = lax.axis_size(axis)
    return lax.ppermute(x, axis, [(i, (i + ahead) % size) for i in range(size)])


def scaled_adapters(side, weights, embedded, totals, gain, before=None):
    groups, columns = gain.shape
    chunks = totals.shape[0]
    tasks = chunks * LANES
    padding = -columns % LANES

    def kernel(side_ref, weights_ref, embedded_ref, totals_ref, gain_ref, *refs):
        out_hbm, out_ref, sems = refs[-3:]
        start = pl.multiple_of(side_ref[0] * tasks, tasks)
        wanted = embedded_ref[pl.ds(start, tasks), :]
        gains = gain_ref[...].astype(jnp.float32)
        gains = jnp.transpose(jnp.concatenate([gains, jnp.zeros((groups, padding), jnp.float32)], axis=1))
        stores = []
        for g in range(groups):
            power = jnp.concatenate([totals_ref[k, g : g + 1, :] for k in range(chunks)], axis=1)
            inverse = lax.rsqrt(power / BLOCK + EPSILON)
            made = lax.dot_general(
                weights_ref[g * columns : (g + 1) * columns, :],
                wanted,
                ROWS_BY_ROWS,
                preferred_element_type=jnp.float32,
            )
            out_ref[g] = (made * inverse * gains[:columns, g : g + 1]).astype(jnp.bfloat16)
            place = out_hbm.at[pl.ds(g * columns, columns), pl.ds(start, tasks)]
            store = pltpu.make_async_copy(out_ref.at[g], place, sems.at[g])
            store.start()
            stores.append(store)
        for store in stores:
            store.wait()

    operands = [side, weights, embedded, totals, gain]
    specs = [SMEM, VMEM, VMEM, VMEM, VMEM]
    aliases = {}
    if before is not None:
        aliases = {len(operands): 0}
        operands.append(before)
        specs.append(HBM)
    return pl.pallas_call(
        kernel,
        out_shape=jax.ShapeDtypeStruct((groups * columns, embedded.shape[0]), jnp.bfloat16),
        in_specs=specs,
        out_specs=HBM,
        scratch_shapes=[pltpu.VMEM((groups, columns, tasks), jnp.bfloat16), pltpu.SemaphoreType.DMA((groups,))],
        input_output_aliases=aliases,
        compiler_params=limit(16),
        name="scale",
    )(*operands)


def on_device(task_ids, task_table, enc_in, enc_out, generator, gain):
    width, groups, columns = generator.shape
    half = task_table.shape[0] // 2
    core = lax.axis_index("core").reshape(1).astype(jnp.int32)
    weights = generator.transpose(1, 2, 0).reshape(groups * columns, width)
    copies = encode_half(core, task_table, enc_in, enc_out, lax.axis_size(PARAM))
    task_ids, copies = lax.optimization_barrier((task_ids, copies))
    mine = exchange(copies, PARAM).reshape(-1, width)
    ids = lax.all_gather(task_ids.reshape(1, -1), TASK, axis=0, tiled=True)
    weights = loaded(weights, ids)
    mine, ids, weights = lax.optimization_barrier((mine, ids, weights))
    low, high = [around(piece, "core", 1) for piece in split_in_two(mine)]
    part = picked(core, ids, mine, half)
    part = picked(1 - core, ids, low, half, 0, part)
    high, part = lax.optimization_barrier((high, part))
    embedded = picked(1 - core, ids, high, half, low.shape[0], part)
    given = squares_of(1 - core, embedded, weights, groups)
    received = around(given, "core", 1)
    kept = squares_of(core, embedded, weights, groups)
    plane = exchange(pair_for_each(kept, received, lax.axis_size(PLANE)), PLANE)
    column = exchange(sum_for_each(plane, lax.axis_size(COLUMN)), COLUMN)
    totals = sum_for_each(column, 1)[0]
    others = around(totals, "core", 1)
    made = scaled_adapters(core, weights, embedded, totals, gain)
    made = scaled_adapters(1 - core, weights, embedded, others, gain, made)
    return made.reshape(groups, columns, -1).transpose(2, 0, 1)


def solution(mesh):
    torus = Mesh(mesh.devices.reshape(8, 4, 4, 2), PARAM_TASK)
    return jax.shard_map(
        on_device,
        mesh=torus,
        in_specs=(
            P(TASK),
            P(PARAM, None),
            P(),
            P(),
            P(None, None, PARAM_TASK),
            P(None, PARAM_TASK),
        ),
        out_specs=P(None, None, PARAM_TASK),
        check_vma=False,
    )
```

```python
import jax
import jax.numpy as jnp
from jax import lax
from jax.experimental import pallas as pl
from jax.experimental.pallas import tpu as pltpu
from jax.sharding import Mesh
from jax.sharding import PartitionSpec as P

BLOCK = 114688
PARAM = ("z", "x")
TASK = ("y", "core")
PARAM_TASK = ("z", "x", "y", "core")
PLANE = ("x", "y")
COLUMN = "z"
LANES = 128
EPSILON = 1e-06

VMEM = pl.BlockSpec(memory_space=pltpu.VMEM)
HBM = pl.BlockSpec(memory_space=pltpu.HBM)
SMEM = pl.BlockSpec(memory_space=pltpu.SMEM)
ROWS_BY_ROWS = (((1,), (1,)), ((), ()))


def in_hbm(x):
    return pltpu.with_memory_space_constraint(x, pltpu.HBM)


def limit(mebibytes):
    return pltpu.CompilerParams(vmem_limit_bytes=mebibytes << 20)


def exchange(x, axis):
    return lax.all_to_all(x, axis, split_axis=0, concat_axis=0, tiled=True)


def copy_for_each(x, axis):
    return exchange(jnp.broadcast_to(x, (lax.axis_size(axis), *x.shape)), axis)


def encode_kernel(core_ref, table_hbm, enc_in_hbm, enc_out_hbm, out_ref, table_ref, enc_in_ref, enc_out_ref, sems):
    copies, rows, _ = out_ref.shape
    start = pl.multiple_of(core_ref[0] * rows, rows)
    loads = [
        pltpu.make_async_copy(table_hbm.at[pl.ds(start, rows), :], table_ref, sems.at[0]),
        pltpu.make_async_copy(enc_in_hbm, enc_in_ref, sems.at[1]),
        pltpu.make_async_copy(enc_out_hbm, enc_out_ref, sems.at[2]),
    ]
    for load in loads:
        load.start()
    loads[0].wait()
    loads[1].wait()
    raw = table_ref[...]
    inner = jax.nn.gelu(jnp.dot(raw, enc_in_ref[...], preferred_element_type=jnp.float32)).astype(jnp.bfloat16)
    loads[2].wait()
    mixed = raw.astype(jnp.float32) + jnp.dot(inner, enc_out_ref[...], preferred_element_type=jnp.float32)
    encoded = mixed.astype(jnp.bfloat16)
    for copy in range(copies):
        out_ref[copy] = encoded


def encode_half(core, task_table, enc_in, enc_out, copies):
    rows, width = task_table.shape[0] // 2, task_table.shape[1]
    return pl.pallas_call(
        encode_kernel,
        out_shape=jax.ShapeDtypeStruct((copies, rows, width), jnp.bfloat16),
        in_specs=[SMEM, HBM, HBM, HBM],
        out_specs=VMEM,
        scratch_shapes=[
            pltpu.VMEM((rows, width), jnp.bfloat16),
            pltpu.VMEM(enc_in.shape, jnp.bfloat16),
            pltpu.VMEM(enc_out.shape, jnp.bfloat16),
            pltpu.SemaphoreType.DMA((3,)),
        ],
        compiler_params=limit(8),
        name="encode_half",
    )(core, in_hbm(task_table), in_hbm(enc_in), in_hbm(enc_out))


def picked_rows(ids_ref, part_ref, which, half):
    chunks = ids_ref.shape[0]
    ids = jnp.transpose(ids_ref[...])
    place = lax.broadcasted_iota(jnp.int32, (1, part_ref.shape[0]), 1)
    labels = (place // half) * (2 * half) + place % half + which * half
    hot = [(ids[:, k : k + 1] == labels).astype(jnp.bfloat16) for k in range(chunks)]
    return jnp.dot(jnp.concatenate(hot, axis=0), part_ref[...], preferred_element_type=jnp.float32)


def first_half(core, ids, mine, weights, half):
    def kernel(core_ref, ids_ref, mine_ref, weights_hbm, part_ref, weights_ref, sem):
        load = pltpu.make_async_copy(weights_hbm, weights_ref, sem)
        load.start()
        part_ref[...] = picked_rows(ids_ref, mine_ref, core_ref[0], half).astype(jnp.bfloat16)
        load.wait()

    return pl.pallas_call(
        kernel,
        out_shape=(
            jax.ShapeDtypeStruct((ids.size, mine.shape[1]), jnp.bfloat16),
            jax.ShapeDtypeStruct(weights.shape, weights.dtype),
        ),
        in_specs=[SMEM, VMEM, VMEM, HBM],
        out_specs=(VMEM, VMEM),
        scratch_shapes=[pltpu.SemaphoreType.DMA],
        compiler_params=limit(16),
        name="first_half",
    )(core, ids, mine, in_hbm(weights))


def embed(core, ids, part, other, half):
    def kernel(core_ref, ids_ref, part_ref, other_ref, embedded_ref):
        rest = picked_rows(ids_ref, other_ref, 1 - core_ref[0], half)
        embedded_ref[...] = (part_ref[...].astype(jnp.float32) + rest).astype(jnp.bfloat16)

    return pl.pallas_call(
        kernel,
        out_shape=jax.ShapeDtypeStruct(part.shape, jnp.bfloat16),
        in_specs=[SMEM, VMEM, VMEM, VMEM],
        out_specs=VMEM,
        compiler_params=limit(16),
        name="embed",
    )(core, ids, part, other)


def squares_of(side, embedded, weights, groups):
    columns = weights.shape[0] // groups
    tasks = embedded.shape[0] // 2
    chunks = tasks // LANES

    def kernel(side_ref, embedded_ref, weights_ref, squares_ref):
        wanted = embedded_ref[pl.ds(pl.multiple_of(side_ref[0] * tasks, tasks), tasks), :]
        for g in range(groups):
            made = lax.dot_general(
                weights_ref[g * columns : (g + 1) * columns, :],
                wanted,
                ROWS_BY_ROWS,
                preferred_element_type=jnp.float32,
            )
            total = jnp.sum(made * made, axis=0, keepdims=True)
            for k in range(chunks):
                squares_ref[k, g : g + 1, :] = total[:, k * LANES : (k + 1) * LANES]

    return pl.pallas_call(
        kernel,
        out_shape=jax.ShapeDtypeStruct((chunks, groups, LANES), jnp.float32),
        in_specs=[SMEM, VMEM, VMEM],
        out_specs=VMEM,
        compiler_params=limit(16),
        name="squares",
    )(side, embedded, weights)


def sum_for_each(pieces, copies):
    def kernel(pieces_ref, out_ref):
        total = pieces_ref[0]
        for i in range(1, pieces_ref.shape[0]):
            total = total + pieces_ref[i]
        for copy in range(copies):
            out_ref[copy] = total

    return pl.pallas_call(
        kernel,
        out_shape=jax.ShapeDtypeStruct((copies, *pieces.shape[1:]), jnp.float32),
        in_specs=[VMEM],
        out_specs=VMEM,
        compiler_params=limit(8),
        name="sum_for_each",
    )(pieces)


def pair_for_each(kept, received, copies):
    def kernel(kept_ref, received_ref, out_ref):
        total = kept_ref[...] + received_ref[...]
        for copy in range(copies):
            out_ref[copy] = total

    return pl.pallas_call(
        kernel,
        out_shape=jax.ShapeDtypeStruct((copies, *kept.shape), jnp.float32),
        in_specs=[VMEM, VMEM],
        out_specs=VMEM,
        compiler_params=limit(8),
        name="pair_for_each",
    )(kept, received)


def around(x, axis, ahead):
    size = lax.axis_size(axis)
    return lax.ppermute(x, axis, [(i, (i + ahead) % size) for i in range(size)])


def scaled_adapters(side, weights, embedded, totals, gain, before=None):
    groups, columns = gain.shape
    chunks = totals.shape[0]
    tasks = chunks * LANES
    padding = -columns % LANES

    def kernel(side_ref, weights_ref, embedded_ref, totals_ref, gain_ref, *refs):
        out_hbm, out_ref, sems = refs[-3:]
        start = pl.multiple_of(side_ref[0] * tasks, tasks)
        wanted = embedded_ref[pl.ds(start, tasks), :]
        gains = gain_ref[...].astype(jnp.float32)
        gains = jnp.transpose(jnp.concatenate([gains, jnp.zeros((groups, padding), jnp.float32)], axis=1))
        stores = []
        for g in range(groups):
            power = jnp.concatenate([totals_ref[k, g : g + 1, :] for k in range(chunks)], axis=1)
            inverse = lax.rsqrt(power / BLOCK + EPSILON)
            made = lax.dot_general(
                weights_ref[g * columns : (g + 1) * columns, :],
                wanted,
                ROWS_BY_ROWS,
                preferred_element_type=jnp.float32,
            )
            out_ref[g] = (made * inverse * gains[:columns, g : g + 1]).astype(jnp.bfloat16)
            place = out_hbm.at[pl.ds(g * columns, columns), pl.ds(start, tasks)]
            store = pltpu.make_async_copy(out_ref.at[g], place, sems.at[g])
            store.start()
            stores.append(store)
        for store in stores:
            store.wait()

    operands = [side, weights, embedded, totals, gain]
    specs = [SMEM, VMEM, VMEM, VMEM, VMEM]
    aliases = {}
    if before is not None:
        aliases = {len(operands): 0}
        operands.append(before)
        specs.append(HBM)
    return pl.pallas_call(
        kernel,
        out_shape=jax.ShapeDtypeStruct((groups * columns, embedded.shape[0]), jnp.bfloat16),
        in_specs=specs,
        out_specs=HBM,
        scratch_shapes=[pltpu.VMEM((groups, columns, tasks), jnp.bfloat16), pltpu.SemaphoreType.DMA((groups,))],
        input_output_aliases=aliases,
        compiler_params=limit(16),
        name="scale",
    )(*operands)


def on_device(task_ids, task_table, enc_in, enc_out, generator, gain):
    width, groups, columns = generator.shape
    half = task_table.shape[0] // 2
    core = lax.axis_index("core").reshape(1).astype(jnp.int32)
    weights = generator.transpose(1, 2, 0).reshape(groups * columns, width)
    copies = encode_half(core, task_table, enc_in, enc_out, lax.axis_size(PARAM))
    task_ids, copies = lax.optimization_barrier((task_ids, copies))
    mine = exchange(copies, PARAM).reshape(-1, width)
    ids = lax.all_gather(task_ids.reshape(1, -1), TASK, axis=0, tiled=True)
    mine, ids = lax.optimization_barrier((mine, ids))
    other = lax.ppermute(mine, "core", [(0, 1), (1, 0)])
    part, weights = first_half(core, ids, mine, weights, half)
    embedded = embed(core, ids, part, other, half)
    given = squares_of(1 - core, embedded, weights, groups)
    received = around(given, "core", 1)
    kept = squares_of(core, embedded, weights, groups)
    column = exchange(pair_for_each(kept, received, lax.axis_size(COLUMN)), COLUMN)
    plane = exchange(sum_for_each(column, lax.axis_size(PLANE)), PLANE)
    totals = sum_for_each(plane, 1)[0]
    others = around(totals, "core", 1)
    made = scaled_adapters(core, weights, embedded, totals, gain)
    made = scaled_adapters(1 - core, weights, embedded, others, gain, made)
    return made.reshape(groups, columns, -1).transpose(2, 0, 1)


def solution(mesh):
    torus = Mesh(mesh.devices.reshape(8, 4, 4, 2), PARAM_TASK)
    return jax.shard_map(
        on_device,
        mesh=torus,
        in_specs=(
            P(TASK),
            P(PARAM, None),
            P(),
            P(),
            P(None, None, PARAM_TASK),
            P(None, PARAM_TASK),
        ),
        out_specs=P(None, None, PARAM_TASK),
        check_vma=False,
    )
```
